32 devices in a mesh: tm: 4 (over y, x), space: 8 (over z, core).
Axes of the slice: x: 2, y: 2, z: 4, core: 2. Of those that a mesh axis runs over, the one named last changes fastest.
Arguments:
- state: float32 [4, 6, 8, 128, 128], P('tm', None, None, 'space'), may hold values from -6 to 6
- multiplier: float32 [4, 6, 8, 128, 128], P('tm', None, None, 'space'), may hold values from -6 to 6
- members: bfloat16 [4, 40, 6, 8, 128, 128], P('tm', None, None, None, 'space'), may hold values from -6 to 6
- static_var: float32 [4, 6, 8, 128, 128], P('tm', None, None, 'space'), may hold values from 0.1 to 1
- courant: float32 [4, 2, 8, 128, 128], P('tm', None, None, 'space'), may hold values from -0.45 to 0.45
- coupling: float32 [8, 6, 6], replicated, may hold values from -2 to 2
- loc_offsets: int32 [9], replicated, may hold values from -8 to 8, as said below
Outputs:
- first_row: float32 [4, 6, 8, 128, 128], P('tm', None, None, 'space')
The draws below stay inside these ranges and needn't reach their ends.
Inputs may be any that keep to these rules, and one draw needn't show every extreme that they name: `loc_offsets`: both -8 and 8 occur among the offsets.
All inputs are finite; a program needn't handle non-finite values.
Results may differ from the reference program's by a relative error of at most 0.0013.
Values may be sent and summed in bfloat16 or wider, within the bound.
No kernel may reach another device: no remote copies, remote signals or barrier semaphores. Data moves between devices by JAX's collectives and lax.ppermute only.
A program may use at most 128 MiB of HBM per device.

```python
import math
import jax
import jax.numpy as jnp
from jax import lax

NV = 6
LEV = 8
MEMBERS = 40
TY = 128
NOFF = 9
RMAX = 8
SUBWIN = 4
NX = 128


def draw_loc_offsets(key, part):
    inner = jax.random.randint(key, (NOFF - 2,), -RMAX, RMAX + 1, dtype=jnp.int32)
    ends = jnp.array([-RMAX, RMAX], jnp.int32)
    joined = jnp.concatenate([ends, inner])
    order = jax.random.permutation(jax.random.fold_in(key, 7), NOFF)
    return joined[order]


def shard_levels(key, shape, split, smallest, top_value):
    level = 1.0
    for axis_at, shards_of in split:
        draws = jax.random.uniform(jax.random.fold_in(jax.random.fold_in(key, 6), axis_at), (shards_of,), jnp.float32, smallest / len(split), top_value / len(split))
        level = level * jnp.repeat(jnp.exp(draws), shape[axis_at] // shards_of).reshape((-1,) + (1,) * (len(shape) - 1 - axis_at))
    return level


def noise(stream_key, dims, deviation, bound, shards=(), kind=jnp.bfloat16):
    level = shard_levels(stream_key, dims, shards, -0.22, 0.18) if shards else 1.0
    values = jax.random.normal(stream_key, dims, jnp.float32) * deviation * level
    return jnp.minimum(jnp.maximum(values, -bound), bound).astype(kind)


def setup_inputs(seed: int = 0) -> dict:
    key_list = jax.random.split(jax.random.key(seed), 8)
    state = noise(key_list[0], (SUBWIN, NV, LEV, NX, TY), 1.0, 6.0, ((0, 4), (3, 8)), jnp.float32)
    multiplier = noise(key_list[1], (SUBWIN, NV, LEV, NX, TY), 1.0, 6.0, ((0, 4), (3, 8)), jnp.float32)
    members = noise(key_list[2], (SUBWIN, MEMBERS, NV, LEV, NX, TY), 1.0, 6.0, ((0, 4), (4, 8)))
    static_var = jnp.clip(jnp.exp(math.log(1.0) - 2.3025851 * jax.random.uniform(key_list[3], (SUBWIN, NV, LEV, NX, TY), jnp.float32) ** shard_levels(key_list[3], (SUBWIN, NV, LEV, NX, TY), ((0, 4), (3, 8)), -0.2, 0.2)), 0.1, 1.0)
    courant = jnp.clip(jax.random.uniform(key_list[4], (SUBWIN, 2, LEV, NX, TY), jnp.float32, -0.45, 0.45) * shard_levels(key_list[4], (SUBWIN, 2, LEV, NX, TY), ((0, 4), (3, 8)), -0.4, 0.0), -0.45, 0.45)
    coupling = noise(key_list[5], (LEV, NV, NV), 0.15, 2.0, (), jnp.float32)
    loc_offsets = draw_loc_offsets(jax.random.fold_in(key_list[7], 71), 0)
    return dict(state=state, multiplier=multiplier, members=members, static_var=static_var, courant=courant, coupling=coupling, loc_offsets=loc_offsets)


def tangent_step(padded, winds, coupling):
    center = padded[:, :, 1:-1]
    west_cells = padded[:, :, :-2]
    east_cells = padded[:, :, 2:]
    zero_row = jnp.zeros_like(center[..., :1])
    south_cells = jnp.concatenate([zero_row, center[..., :-1]], axis=-1)
    north_cells = jnp.concatenate([center[..., 1:], zero_row], axis=-1)
    courant_x = winds[0]
    courant_y = winds[1]
    advection = jnp.maximum(courant_x, 0.0) * (center - west_cells)
    advection = advection + jnp.minimum(courant_x, 0.0) * (east_cells - center)
    advection = advection + jnp.maximum(courant_y, 0.0) * (center - south_cells)
    advection = advection + jnp.minimum(courant_y, 0.0) * (north_cells - center)
    coupling_term = jnp.einsum("lvw,wlxy->vlxy", coupling, center, precision=lax.Precision.HIGHEST)
    return center - advection + coupling_term


def periodic_step(field, winds, coupling):
    padded = jnp.concatenate([field[:, :, -1:], field, field[:, :, :1]], axis=2)
    return tangent_step(padded, winds, coupling)


def reference(state, multiplier, members, static_var, courant, coupling, loc_offsets):
    weights = jnp.exp(-0.5 * (loc_offsets.astype(jnp.float32) / RMAX) ** 2)
    results = []
    for window in range(SUBWIN):
        lagrange = multiplier[window]
        ensemble = members[window]
        products = (ensemble.astype(jnp.float32) * lagrange[None]).astype(jnp.bfloat16)
        padded = jnp.concatenate([products[:, :, :, -RMAX:], products, products[:, :, :, :RMAX]], axis=3)

        def add_offset(index, total):
            offset_start = (RMAX + loc_offsets[index]).astype(jnp.int32)
            shifted = lax.dynamic_slice_in_dim(padded, offset_start, NX, 3)
            summed = jnp.sum(ensemble.astype(jnp.float32) * shifted.astype(jnp.float32), axis=0)
            return total + weights[index] * summed

        total = lax.fori_loop(0, NOFF, add_offset, jnp.zeros(lagrange.shape, jnp.float32))
        localized = total / (MEMBERS - 1)
        result = 0.5 * static_var[window] * lagrange + 0.5 * localized + state[window]
        if window >= 1:
            propagated = periodic_step(state[window - 1], courant[window], coupling)
            propagated = periodic_step(propagated, courant[window], coupling)
            result = result - propagated
        results.append(result)
    return jnp.stack(results)
```

```python
import functools

import jax
import jax.numpy as jnp
from jax import lax
from jax.experimental import pallas as pl
from jax.experimental.pallas import tpu as pltpu
from jax.sharding import PartitionSpec as P


BLOCK = 256


def ring(axis, distance):
    size = lax.axis_size(axis)
    return [(i, (i + distance) % size) for i in range(size)]


def grouped(members, rows):
    group = max(1, BLOCK // rows)
    while members % group:
        group -= 1
    return group


def weights_kernel(span, offsets_ref, out_ref):
    size = out_ref.shape[-1]
    row = lax.broadcasted_iota(jnp.int32, (size, size), 0)
    col = lax.broadcasted_iota(jnp.int32, (size, size), 1)
    shift = col - row
    half = span // 2
    same_block = (row // span) == (col // span)
    count = jnp.zeros((size, size), jnp.float32)
    for j in range(offsets_ref.shape[0]):
        count = count + jnp.where(shift == offsets_ref[j], 1.0, 0.0)
    scaled = shift.astype(jnp.float32) * (1.0 / half)
    weight = jnp.where(same_block, count * jnp.exp(-0.5 * scaled * scaled), 0.0)
    across = jnp.where((row // half) != (col // half), weight, 0.0)
    for k, matrix in enumerate((weight, across)):
        high = matrix.astype(jnp.bfloat16)
        out_ref[2 * k] = high
        out_ref[2 * k + 1] = (matrix - high.astype(jnp.float32)).astype(jnp.bfloat16)


def band_weights(loc_offsets, span, size):
    return pl.pallas_call(
        functools.partial(weights_kernel, span),
        out_shape=jax.ShapeDtypeStruct((4, size, size), jnp.bfloat16),
        in_specs=[pl.BlockSpec(memory_space=pltpu.SMEM)],
        out_specs=pl.BlockSpec(memory_space=pltpu.VMEM),
        name="weights",
    )(loc_offsets)


def smoothed_pairs(high, low, fields, lam, group):
    rows = lam.shape[0]
    block = jnp.concatenate(fields, axis=0) if group > 1 else fields[0]
    lams = jnp.concatenate([lam] * group, axis=0) if group > 1 else lam
    products = (block * lams).astype(jnp.bfloat16)
    smooth = jnp.dot(high, products, preferred_element_type=jnp.float32)
    smooth = smooth + jnp.dot(low, products, preferred_element_type=jnp.float32)
    pairs = block * smooth
    total = pairs[:rows]
    for g in range(1, group):
        total = total + pairs[g * rows : (g + 1) * rows]
    return total


def interior_kernel(group, w_ref, m_ref, lam_ref, out_ref):
    members = m_ref.shape[0]
    lam = lam_ref[0]
    high, low = w_ref[0], w_ref[1]

    def step(i, total):
        fields = [m_ref[i * group + g, 0].astype(jnp.float32) for g in range(group)]
        return total + smoothed_pairs(high, low, fields, lam, group)

    out_ref[0] = lax.fori_loop(0, members // group, step, jnp.zeros(lam.shape, jnp.float32), unroll=4)


def interior(weights, ensemble, lagrange, group):
    members, nv, rows, ty = ensemble.shape
    size = weights.shape[-1]
    return pl.pallas_call(
        functools.partial(interior_kernel, group),
        grid=(nv,),
        out_shape=jax.ShapeDtypeStruct((nv, rows, ty), jnp.float32),
        in_specs=[
            pl.BlockSpec((2, size, size), lambda v: (0, 0, 0)),
            pl.BlockSpec((members, 1, rows, ty), lambda v: (0, v, 0, 0)),
            pl.BlockSpec((1, rows, ty), lambda v: (v, 0, 0)),
        ],
        out_specs=pl.BlockSpec((1, rows, ty), lambda v: (v, 0, 0)),
        cost_estimate=pl.CostEstimate(flops=40_000_000_000, bytes_accessed=2 * ensemble.size, transcendentals=0),
        name="interior",
    )(weights, ensemble, lagrange)


def joined(first, second):
    levels, half, ty = first.shape
    both = jnp.concatenate([first[:, None], second[:, None]], axis=1)
    return both.reshape(levels * 2 * half, ty)


def across_kernel(group, w_ref, up_ref, ma_ref, la_ref, dn_ref, mb_ref, lb_ref, own_a, ret_a, own_b, ret_b):
    members = ma_ref.shape[0]
    levels, half, ty = own_a.shape[1:]
    high, low = w_ref[0], w_ref[1]

    def level_rows(ref, index):
        return ref[index].astype(jnp.float32).reshape(levels, half, ty)

    lam_a = joined(level_rows(up_ref.at[0], members), la_ref[0].reshape(levels, half, ty))
    lam_b = joined(lb_ref[0].reshape(levels, half, ty), level_rows(dn_ref.at[0], members))

    def step(i, totals):
        total_a, total_b = totals
        fields_a = []
        fields_b = []
        for g in range(group):
            m = i * group + g
            fields_a.append(joined(level_rows(up_ref.at[0], m), ma_ref[m, 0].astype(jnp.float32)))
            fields_b.append(joined(mb_ref[m, 0].astype(jnp.float32), level_rows(dn_ref.at[0], m)))
        total_a = total_a + smoothed_pairs(high, low, fields_a, lam_a, group)
        total_b = total_b + smoothed_pairs(high, low, fields_b, lam_b, group)
        return total_a, total_b

    zero = jnp.zeros(lam_a.shape, jnp.float32)
    total_a, total_b = lax.fori_loop(0, members // group, step, (zero, zero), unroll=2)
    total_a = total_a.reshape(levels, 2, half, ty)
    total_b = total_b.reshape(levels, 2, half, ty)
    ret_a[0] = total_a[:, 0].astype(ret_a.dtype).reshape(levels * half, ty)
    own_a[0] = total_a[:, 1]
    own_b[0] = total_b[:, 0]
    ret_b[0] = total_b[:, 1].astype(ret_b.dtype).reshape(levels * half, ty)


def across(weights, from_left, from_right, ensemble, lagrange, first_a, first_b, group):
    members, nv, levels, span, ty = ensemble.shape
    half = span // 2
    count = from_left.shape[0]
    size = weights.shape[-1]
    halves = (members, 1, levels, half, ty)
    halo = pl.BlockSpec((1, members + 1, levels * half, ty), lambda v: (v, 0, 0, 0))
    own_spec = pl.BlockSpec((1, levels, half, ty), lambda v: (v, 0, 0, 0))
    ret_spec = pl.BlockSpec((1, levels * half, ty), lambda v: (v, 0, 0))
    own_type = jax.ShapeDtypeStruct((count, levels, half, ty), jnp.float32)
    ret_type = jax.ShapeDtypeStruct((count, levels * half, ty), jnp.bfloat16)
    return pl.pallas_call(
        functools.partial(across_kernel, group),
        grid=(count,),
        out_shape=(own_type, ret_type, own_type, ret_type),
        in_specs=[
            pl.BlockSpec((2, size, size), lambda v: (1, 0, 0)),
            halo,
            pl.BlockSpec(halves, lambda v: (0, first_a + v, 0, 0, 0)),
            pl.BlockSpec((1, levels, half, ty), lambda v: (first_a + v, 0, 0, 0)),
            halo,
            pl.BlockSpec(halves, lambda v: (0, first_b + v, 0, 1, 0)),
            pl.BlockSpec((1, levels, half, ty), lambda v: (first_b + v, 0, 1, 0)),
        ],
        out_specs=(own_spec, ret_spec, own_spec, ret_spec),
        cost_estimate=pl.CostEstimate(flops=10_000_000_000 * count, bytes_accessed=2 * ensemble.size, transcendentals=0),
        name="across",
    )(weights, from_left, ensemble, lagrange, from_right, ensemble, lagrange)


def pack_kernel(ma_ref, la_ref, mb_ref, lb_ref, up_ref, dn_ref):
    members = ma_ref.shape[0]
    rows, ty = up_ref.shape[2:]
    up_ref[0, :members] = ma_ref[:, 0].reshape(members, rows, ty)
    up_ref[0, members] = la_ref[0].astype(up_ref.dtype).reshape(rows, ty)
    dn_ref[0, :members] = mb_ref[:, 0].reshape(members, rows, ty)
    dn_ref[0, members] = lb_ref[0].astype(dn_ref.dtype).reshape(rows, ty)


def packed(ensemble, lagrange, first_a, first_b, count):
    members, nv, levels, span, ty = ensemble.shape
    half = span // 2
    halves = (members, 1, levels, half, ty)
    out_spec = pl.BlockSpec((1, members + 1, levels * half, ty), lambda v: (v, 0, 0, 0))
    out_type = jax.ShapeDtypeStruct((count, members + 1, levels * half, ty), jnp.bfloat16)
    return pl.pallas_call(
        pack_kernel,
        grid=(count,),
        out_shape=(out_type, out_type),
        in_specs=[
            pl.BlockSpec(halves, lambda v: (0, first_a + v, 0, 1, 0)),
            pl.BlockSpec((1, levels, half, ty), lambda v: (first_a + v, 0, 1, 0)),
            pl.BlockSpec(halves, lambda v: (0, first_b + v, 0, 0, 0)),
            pl.BlockSpec((1, levels, half, ty), lambda v: (first_b + v, 0, 0, 0)),
        ],
        out_specs=(out_spec, out_spec),
        name="pack",
    )(ensemble, lagrange, ensemble, lagrange)


def tangent_step(padded, winds, coupling):
    center = padded[:, :, 1:-1]
    west_cells = padded[:, :, :-2]
    east_cells = padded[:, :, 2:]
    zero_row = jnp.zeros_like(center[..., :1])
    south_cells = jnp.concatenate([zero_row, center[..., :-1]], axis=-1)
    north_cells = jnp.concatenate([center[..., 1:], zero_row], axis=-1)
    courant_x = winds[0]
    courant_y = winds[1]
    advection = jnp.maximum(courant_x, 0.0) * (center - west_cells)
    advection = advection + jnp.minimum(courant_x, 0.0) * (east_cells - center)
    advection = advection + jnp.maximum(courant_y, 0.0) * (center - south_cells)
    advection = advection + jnp.minimum(courant_y, 0.0) * (north_cells - center)
    coupling_term = jnp.einsum("lvw,wlxy->vlxy", coupling, center, precision=lax.Precision.HIGHEST)
    return center - advection + coupling_term


def per_device(state, multiplier, members, static_var, courant, coupling, loc_offsets):
    own_state = state[0]
    lagrange = multiplier[0]
    ensemble = members[0]
    variance = static_var[0]
    own_winds = courant[0]
    count, nv, levels, span, ty = ensemble.shape
    half = span // 2
    pairs = nv // 2
    up, down = ring("space", 1), ring("space", -1)
    later = [(i, i + 1) for i in range(lax.axis_size("tm") - 1)]

    from_left, from_right = [], []
    for c in range(pairs):
        to_right, to_left = packed(ensemble, lagrange, c, pairs + c, 1)
        from_left.append(lax.ppermute(to_right, "space", up))
        from_right.append(lax.ppermute(to_left, "space", down))

    earlier = lax.ppermute(own_state, "tm", later)
    edge = lambda array, width, low: array[:, :, :width] if low else array[:, :, span - width :]
    states_left = lax.ppermute(edge(earlier, 2, False), "space", up)
    states_right = lax.ppermute(edge(earlier, 2, True), "space", down)
    winds_left = lax.ppermute(edge(own_winds, 1, False), "space", up)
    winds_right = lax.ppermute(edge(own_winds, 1, True), "space", down)

    rows = levels * span
    group = grouped(count, rows)
    weights = band_weights(loc_offsets, span, group * rows)
    inner = interior(weights, ensemble.reshape(count, nv, rows, ty), lagrange.reshape(nv, rows, ty), group)

    padded_state = jnp.concatenate([states_left, earlier, states_right], axis=2)
    padded_winds = jnp.concatenate([winds_left, own_winds, winds_right], axis=2)
    halfway = tangent_step(padded_state, padded_winds, coupling)
    propagated = tangent_step(halfway, own_winds, coupling)
    base = 0.5 * variance * lagrange + own_state - propagated

    own_as, own_bs, back_as, back_bs = [], [], [], []
    for c in range(pairs):
        own_a, ret_a, own_b, ret_b = across(
            weights, from_left[c], from_right[c], ensemble, lagrange, c, pairs + c, group
        )
        own_as.append(own_a)
        own_bs.append(own_b)
        back_as.append(lax.ppermute(ret_a, "space", down))
        back_bs.append(lax.ppermute(ret_b, "space", up))
    wide = lambda parts: jnp.concatenate(parts, axis=0).astype(jnp.float32).reshape(pairs, levels, half, ty)
    cross_a = jnp.concatenate([wide(own_as), wide(back_as)], axis=2)
    cross_b = jnp.concatenate([wide(back_bs), wide(own_bs)], axis=2)
    cross = jnp.concatenate([cross_a, cross_b], axis=0)
    total = inner.reshape(nv, levels, span, ty) + cross
    return (base + (0.5 / (count - 1)) * total)[None]


def solution(mesh):
    return jax.shard_map(
        per_device,
        mesh=mesh,
        in_specs=(
            P("tm", None, None, "space", None),
            P("tm", None, None, "space", None),
            P("tm", None, None, None, "space", None),
            P("tm", None, None, "space", None),
            P("tm", None, None, "space", None),
            P(),
            P(),
        ),
        out_specs=P("tm", None, None, "space", None),
        check_vma=False,
    )
```

```python
import functools

import jax
import jax.numpy as jnp
from jax import lax
from jax.experimental import pallas as pl
from jax.experimental.pallas import tpu as pltpu
from jax.sharding import PartitionSpec as P


BAND = 128
SPLIT = 2
TILE = 8
GRANT = 16 * 1024 * 1024


def ring(axis, distance):
    size = lax.axis_size(axis)
    return [(i, (i + distance) % size) for i in range(size)]


def divisor(number, limit):
    while number % limit:
        limit -= 1
    return limit


def weights_kernel(span, offsets_ref, out_ref):
    size = out_ref.shape[1]
    row = lax.broadcasted_iota(jnp.int32, (size, size), 0)
    col = lax.broadcasted_iota(jnp.int32, (size, size), 1)
    shift = col - row
    half = span // 2
    same_block = (row // span) == (col // span)
    count = jnp.zeros((size, size), jnp.float32)
    for j in range(offsets_ref.shape[0]):
        count = count + jnp.where(shift == offsets_ref[j], 1.0, 0.0)
    scaled = shift.astype(jnp.float32) * (1.0 / half)
    weight = jnp.where(same_block, count * jnp.exp(-0.5 * scaled * scaled), 0.0)
    across = jnp.where((row // half) != (col // half), weight, 0.0)
    for k, matrix in enumerate((weight, across)):
        high = matrix.astype(jnp.bfloat16)
        out_ref[k, :, :size] = high
        out_ref[k, :, size:] = (matrix - high.astype(jnp.float32)).astype(jnp.bfloat16)


def band_weights(loc_offsets, span, size):
    return pl.pallas_call(
        functools.partial(weights_kernel, span),
        out_shape=jax.ShapeDtypeStruct((2, size, 2 * size), jnp.bfloat16),
        in_specs=[pl.BlockSpec(memory_space=pltpu.SMEM)],
        out_specs=pl.BlockSpec(memory_space=pltpu.VMEM),
        name="weights",
    )(loc_offsets)


def shapes_of_matmul(members, rows):
    stacked = divisor(members, max(1, BAND // rows))
    beside = divisor(members // stacked, 2)
    return stacked, beside


def smoothed_pairs(weights, fields, lam):
    rows, ty = lam.shape
    products = [
        jnp.concatenate([(field * lam).astype(jnp.bfloat16) for field in column], axis=0)
        for column in fields
    ]
    products = jnp.concatenate(products, axis=1)
    smooth = jnp.dot(
        weights, jnp.concatenate([products, products], axis=0), preferred_element_type=jnp.float32
    )
    total = None
    for b, column in enumerate(fields):
        for s, field in enumerate(column):
            pair = field * smooth[s * rows : (s + 1) * rows, b * ty : (b + 1) * ty]
            total = pair if total is None else total + pair
    return total


def interior_kernel(stacked, beside, w_ref, m_ref, lam_ref, out_ref):
    members, nv = m_ref.shape[:2]
    weights = w_ref[0]
    step = stacked * beside

    def variable(v, carry):
        lam = lam_ref[v]
        total = jnp.zeros(lam.shape, jnp.float32)
        for first in range(0, members, step):
            fields = [
                [m_ref[first + b * stacked + s, v].astype(jnp.float32) for s in range(stacked)]
                for b in range(beside)
            ]
            total = total + smoothed_pairs(weights, fields, lam)
        out_ref[v] = total
        return carry

    lax.fori_loop(0, nv, variable, 0)


def vmem():
    return pl.BlockSpec(memory_space=pltpu.VMEM)


def interior(weights, ensemble, lagrange):
    members, nv, rows, ty = ensemble.shape
    stacked, beside = shapes_of_matmul(members, rows)
    return pl.pallas_call(
        functools.partial(interior_kernel, stacked, beside),
        out_shape=jax.ShapeDtypeStruct((nv, rows, ty), jnp.float32),
        in_specs=[vmem()] * 3,
        out_specs=vmem(),
        compiler_params=pltpu.CompilerParams(vmem_limit_bytes=GRANT),
        cost_estimate=pl.CostEstimate(flops=30_000_000_000, bytes_accessed=2 * ensemble.size, transcendentals=0),
        name="interior",
    )(weights, ensemble, lagrange)


def joined(first, second):
    levels, half, ty = first.shape
    both = jnp.concatenate([first[:, None], second[:, None]], axis=1)
    return both.reshape(levels * 2 * half, ty)


def across_kernel(stacked, beside, first_unit, w_ref, up_ref, dn_ref, m_ref, lam_ref, own_a, ret_a, own_b, ret_b):
    members, nv = m_ref.shape[:2]
    number, levels, half, ty = own_a.shape
    span = 2 * half
    pairs = nv // 2
    weights = w_ref[1]

    def unit(u, carry):
        v = (first_unit + u) // SPLIT
        row = (first_unit + u) % SPLIT * levels * span
        rows = pl.ds(pl.multiple_of(row, levels * span), levels * span)

        def halo(ref, index):
            return ref[u, index].astype(jnp.float32)

        def own(block, side):
            block = block.astype(jnp.float32).reshape(levels, 2, half, ty)
            return block[:, side]

        lam_a = joined(halo(up_ref, members), own(lam_ref[v, rows], 0))
        lam_b = joined(own(lam_ref[pairs + v, rows], 1), halo(dn_ref, members))
        total_a = jnp.zeros(lam_a.shape, jnp.float32)
        total_b = jnp.zeros(lam_b.shape, jnp.float32)
        for first in range(0, members, stacked * beside):
            indices = [[first + b * stacked + s for s in range(stacked)] for b in range(beside)]
            fields = [[joined(halo(up_ref, m), own(m_ref[m, v, rows], 0)) for m in column] for column in indices]
            total_a = total_a + smoothed_pairs(weights, fields, lam_a)
            fields = [[joined(own(m_ref[m, pairs + v, rows], 1), halo(dn_ref, m)) for m in column] for column in indices]
            total_b = total_b + smoothed_pairs(weights, fields, lam_b)
        total_a = total_a.reshape(levels, 2, half, ty)
        total_b = total_b.reshape(levels, 2, half, ty)
        ret_a[u] = total_a[:, 0].astype(ret_a.dtype)
        own_a[u] = total_a[:, 1]
        own_b[u] = total_b[:, 0]
        ret_b[u] = total_b[:, 1].astype(ret_b.dtype)
        return carry

    if number == 1:
        unit(0, 0)
    else:
        lax.fori_loop(0, number, unit, 0)


def across(weights, from_left, from_right, ensemble, lagrange, first):
    members, _, _, ty = ensemble.shape
    number, _, levels, half, _ = from_left.shape
    stacked, beside = shapes_of_matmul(members, levels * 2 * half)
    own_type = jax.ShapeDtypeStruct((number, levels, half, ty), jnp.float32)
    ret_type = jax.ShapeDtypeStruct((number, levels, half, ty), jnp.bfloat16)
    return pl.pallas_call(
        functools.partial(across_kernel, stacked, beside, first),
        out_shape=(own_type, ret_type, own_type, ret_type),
        in_specs=[vmem()] * 5,
        out_specs=(vmem(),) * 4,
        compiler_params=pltpu.CompilerParams(vmem_limit_bytes=GRANT),
        cost_estimate=pl.CostEstimate(flops=5_000_000_000 * number, bytes_accessed=ensemble.size // 3, transcendentals=0),
        name="across",
    )(weights, from_left, from_right, ensemble, lagrange)


def pack_kernel(pieces, m_ref, lam_ref, *refs):
    outs, (lam_up, lam_dn, sem) = refs[:-3], refs[-3:]
    members, nv, _, span, _ = m_ref.shape
    half = span // 2
    levels = outs[0].shape[2]
    pairs = nv // 2
    copies = []
    slot = 0
    for piece, (first, number) in enumerate(pieces):
        for u in range(number):
            v, level = (first + u) // SPLIT, (first + u) % SPLIT * levels
            for side, (var, column, lam_buffer) in enumerate(((v, half, lam_up), (pairs + v, 0, lam_dn))):
                out = outs[2 * piece + side]
                at = (pl.ds(level, levels), pl.ds(column, half))
                copies.append(pltpu.make_async_copy(lam_ref.at[(var,) + at], lam_buffer.at[slot], sem.at[len(copies)]))
                copies.append(
                    pltpu.make_async_copy(
                        m_ref.at[(slice(None), var) + at], out.at[u, pl.ds(0, members)], sem.at[len(copies)]
                    )
                )
            slot += 1
    for copy in copies:
        copy.start()
    slot = 0
    for copy in copies[::2]:
        copy.wait()
    for piece, (first, number) in enumerate(pieces):
        for u in range(number):
            for side, lam_buffer in enumerate((lam_up, lam_dn)):
                out = outs[2 * piece + side]
                out[u, members] = lam_buffer[slot].astype(out.dtype)
            slot += 1
    for copy in copies[1::2]:
        copy.wait()


def packed(ensemble, lagrange, pieces):
    members, _, levels, span, ty = ensemble.shape
    half = span // 2
    levels = levels // SPLIT
    types = []
    for _, number in pieces:
        types += [jax.ShapeDtypeStruct((number, members + 1, levels, half, ty), jnp.bfloat16)] * 2
    units = sum(number for _, number in pieces)
    ensemble = pltpu.with_memory_space_constraint(ensemble, pltpu.HBM)
    lagrange = pltpu.with_memory_space_constraint(lagrange, pltpu.HBM)
    hbm = pl.BlockSpec(memory_space=pltpu.HBM)
    return pl.pallas_call(
        functools.partial(pack_kernel, pieces),
        out_shape=tuple(types),
        in_specs=[hbm, hbm],
        out_specs=(vmem(),) * len(types),
        scratch_shapes=[
            pltpu.VMEM((units, levels, half, ty), jnp.float32),
            pltpu.VMEM((units, levels, half, ty), jnp.float32),
            pltpu.SemaphoreType.DMA((4 * units,)),
        ],
        compiler_params=pltpu.CompilerParams(vmem_limit_bytes=GRANT),
        name="pack",
    )(ensemble, lagrange)


def propagate_kernel(c_ref, e_ref, left_ref, right_ref, w_ref, var_ref, lam_ref, state_ref, out_ref, field_ref, wind_ref):
    nv, levels, span, ty = e_ref.shape
    rows = span + 2 * TILE
    field_ref[...] = jnp.zeros_like(field_ref)
    wind_ref[...] = jnp.zeros_like(wind_ref)
    lane = lax.broadcasted_iota(jnp.int32, (rows, ty), 1)

    def one_level(level, carry):
        for v in range(nv):
            field_ref[v, TILE - 2 : TILE] = left_ref[level, 2 * v : 2 * v + 2]
            field_ref[v, TILE : TILE + span] = e_ref[v, level]
            field_ref[v, TILE + span : TILE + span + 2] = right_ref[level, 2 * v : 2 * v + 2]
        for d in range(2):
            wind_ref[d, TILE - 1 : TILE] = left_ref[level, 2 * nv + d : 2 * nv + d + 1]
            wind_ref[d, TILE : TILE + span] = w_ref[d, level]
            wind_ref[d, TILE + span : TILE + span + 1] = right_ref[level, 2 * nv + d : 2 * nv + d + 1]
        cx, cy = wind_ref[0], wind_ref[1]
        cx_plus, cx_minus = jnp.maximum(cx, 0.0), jnp.minimum(cx, 0.0)
        cy_plus, cy_minus = jnp.maximum(cy, 0.0), jnp.minimum(cy, 0.0)
        fields = [field_ref[v] for v in range(nv)]
        for _ in range(2):
            results = []
            for v in range(nv):
                f = fields[v]
                west = pltpu.roll(f, 1, 0)
                east = pltpu.roll(f, rows - 1, 0)
                south = jnp.where(lane == 0, 0.0, pltpu.roll(f, 1, 1))
                north = jnp.where(lane == ty - 1, 0.0, pltpu.roll(f, ty - 1, 1))
                moved = cx_plus * (f - west) + cx_minus * (east - f)
                moved = moved + cy_plus * (f - south) + cy_minus * (north - f)
                mixed = c_ref[level, v, 0] * fields[0]
                for w in range(1, nv):
                    mixed = mixed + c_ref[level, v, w] * fields[w]
                results.append(f - moved + mixed)
            fields = results
        for v in range(nv):
            local = 0.5 * var_ref[v, level] * lam_ref[v, level] + state_ref[v, level]
            out_ref[v, level] = local - fields[v][TILE : TILE + span]
        return carry

    lax.fori_loop(0, levels, one_level, 0)


def propagate(coupling, earlier, left, right, winds, variance, lagrange, state):
    nv, _, span, ty = earlier.shape
    rows = span + 2 * TILE
    return pl.pallas_call(
        propagate_kernel,
        out_shape=jax.ShapeDtypeStruct(earlier.shape, jnp.float32),
        in_specs=[pl.BlockSpec(memory_space=pltpu.SMEM)] + [vmem()] * 7,
        out_specs=vmem(),
        scratch_shapes=[pltpu.VMEM((nv, rows, ty), jnp.float32), pltpu.VMEM((2, rows, ty), jnp.float32)],
        compiler_params=pltpu.CompilerParams(vmem_limit_bytes=GRANT),
        cost_estimate=pl.CostEstimate(flops=10_000_000_000, bytes_accessed=20 * earlier.size, transcendentals=0),
        name="propagate",
    )(coupling, earlier, left, right, winds, variance, lagrange, state)


def final_kernel(scale, counts, base_ref, inner_ref, *refs):
    out_ref = refs[-1]
    nv, levels, span, _ = out_ref.shape
    half = span // 2
    pairs = nv // 2
    part = levels // SPLIT
    unit = 0
    for c, number in enumerate(counts):
        own_a, own_b, back_a, back_b = refs[4 * c : 4 * c + 4]
        for u in range(number):
            v, first = unit // SPLIT, (unit % SPLIT) * part
            at = pl.ds(first, part)
            for var, low, high in (
                (v, own_a[u], back_a[u].astype(jnp.float32)),
                (pairs + v, back_b[u].astype(jnp.float32), own_b[u]),
            ):
                out_ref[var, at, :half] = base_ref[var, at, :half] + scale * (inner_ref[var, at, :half] + low)
                out_ref[var, at, half:] = base_ref[var, at, half:] + scale * (inner_ref[var, at, half:] + high)
            unit += 1


def final(scale, counts, base, inner, parts):
    return pl.pallas_call(
        functools.partial(final_kernel, scale, counts),
        out_shape=jax.ShapeDtypeStruct(base.shape, jnp.float32),
        in_specs=[vmem()] * (2 + len(parts)),
        out_specs=vmem(),
        compiler_params=pltpu.CompilerParams(vmem_limit_bytes=GRANT),
        name="final",
    )(base, inner, *parts)


def per_device(state, multiplier, members, static_var, courant, coupling, loc_offsets):
    own_state = state[0]
    lagrange = multiplier[0]
    ensemble = members[0]
    own_winds = courant[0]
    count, nv, levels, span, ty = ensemble.shape
    rows = levels * span
    flat_members = ensemble.reshape(count, nv, rows, ty)
    flat_lagrange = lagrange.reshape(nv, rows, ty)
    units = nv // 2 * SPLIT
    up, down = ring("space", 1), ring("space", -1)
    later = [(i, i + 1) for i in range(lax.axis_size("tm") - 1)]
    counts = [units // 3, units - units // 3 - units // 6, units // 6]
    firsts = [sum(counts[:c]) for c in range(len(counts))]
    pieces = list(zip(firsts, counts))

    def edges(low):
        take = lambda array, width: array[:, :, :width] if low else array[:, :, span - width :]
        fields = jnp.swapaxes(take(own_state, 2), 0, 1).reshape(levels, 2 * nv, ty)
        winds = jnp.swapaxes(take(own_winds, 1), 0, 1).reshape(levels, 2, ty)
        return jnp.concatenate([fields, winds], axis=1)

    messages = list(packed(ensemble, lagrange, tuple(pieces[:1])))
    messages += packed(ensemble, lagrange, tuple(pieces[1:]))
    from_left = [lax.ppermute(messages[2 * c], "space", up) for c in range(len(pieces))]
    from_right = [lax.ppermute(messages[2 * c + 1], "space", down) for c in range(len(pieces))]
    left = lax.ppermute(edges(False), "space", up)
    right = lax.ppermute(edges(True), "space", down)
    weights = band_weights(loc_offsets, span, max(rows, BAND))
    inner = interior(weights, flat_members, flat_lagrange)
    own_rows = jnp.swapaxes(own_state, 0, 1).reshape(levels, nv * span, ty)
    sent = jnp.concatenate([own_rows, left[:, : 2 * nv], right[:, : 2 * nv]], axis=1)
    came = lax.ppermute(sent, "tm", later)
    earlier = jnp.swapaxes(came[:, : nv * span].reshape(levels, nv, span, ty), 0, 1)
    edge_left = jnp.concatenate([came[:, nv * span : nv * (span + 2)], left[:, 2 * nv :]], axis=1)
    edge_right = jnp.concatenate([came[:, nv * (span + 2) :], right[:, 2 * nv :]], axis=1)
    base = propagate(coupling, earlier, edge_left, edge_right, own_winds, static_var[0], lagrange, own_state)
    parts = []
    for c in range(len(pieces)):
        own_a, ret_a, own_b, ret_b = across(
            weights, from_left[c], from_right[c], flat_members, flat_lagrange, firsts[c]
        )
        parts += [own_a, own_b, lax.ppermute(ret_a, "space", down), lax.ppermute(ret_b, "space", up)]
    result = final(0.5 / (count - 1), counts, base, inner.reshape(base.shape), parts)
    return result[None]


def solution(mesh):
    return jax.shard_map(
        per_device,
        mesh=mesh,
        in_specs=(
            P("tm", None, None, "space", None),
            P("tm", None, None, "space", None),
            P("tm", None, None, None, "space", None),
            P("tm", None, None, "space", None),
            P("tm", None, None, "space", None),
            P(),
            P(),
        ),
        out_specs=P("tm", None, None, "space", None),
        check_vma=False,
    )
```
